32 devices in a mesh: rows: 2 (over core), cols: 4 (over z), slabs: 4 (over y, x).
Axes of the slice: x: 2, y: 2, z: 4, core: 2. Of those that a mesh axis runs over, the one named last changes fastest.
Arguments:
- density: float32 [32, 384, 32, 128], P('rows', 'cols', 'slabs'), may hold values from 0.5 to 2
- flow_j: float32 [32, 384, 32, 128], P('rows', 'cols', 'slabs'), may hold values from -0.3 to 0.3
- flow_i: float32 [32, 384, 32, 128], P('rows', 'cols', 'slabs'), may hold values from -0.3 to 0.3
- flow_k: float32 [32, 384, 32, 128], P('rows', 'cols', 'slabs'), may hold values from -0.3 to 0.3
Outputs:
- anomaly: float32 [32, 384, 32, 128], P('rows', 'cols', 'slabs')
- density_end: float32 [32, 384, 32, 128], P('rows', 'cols', 'slabs')
The draws below stay inside these ranges and needn't reach their ends.
All inputs are finite; a program needn't handle non-finite values.
Results may differ from the reference program's by a relative error of at most 0.00002.
Values sent between devices are 32-bit elements; how exact they have to be, the bound alone decides.
A program may use at most 128 MiB of HBM per device.

```python
import jax
import jax.numpy as jnp
from jax import lax

GRID_J = 32
GRID_I = 384
GRID_K = 32
LEVELS = 128
STEPS = 6


def block_scale(own_key, extent, shards, least, top_value):
    def one(dim, shards_of):
        steps = jax.random.uniform(jax.random.fold_in(jax.random.fold_in(own_key, 6), dim), (shards_of,), jnp.float32, least / len(shards), top_value / len(shards))
        return jnp.repeat(jnp.exp(steps), extent[dim] // shards_of).reshape((-1,) + (1,) * (len(extent) - dim - 1))

    factor_of = one(*shards[0])
    for cut in shards[1:]:
        factor_of = factor_of * one(*cut)
    return factor_of


def setup_inputs(seed: int = 0) -> dict:
    key_of = jax.random.split(jax.random.key(seed), 5)
    density = jnp.clip(0.5 + 1.5 * jax.random.uniform(key_of[0], (GRID_J, GRID_I, GRID_K, LEVELS), jnp.float32) ** block_scale(key_of[0], (GRID_J, GRID_I, GRID_K, LEVELS), ((0, 2), (1, 4), (2, 4)), -0.2, 0.2), 0.5, 2.0)
    flow_j = jnp.clip(jax.random.uniform(key_of[1], (GRID_J, GRID_I, GRID_K, LEVELS), jnp.float32, -0.3, 0.3) * block_scale(key_of[1], (GRID_J, GRID_I, GRID_K, LEVELS), ((0, 2), (1, 4), (2, 4)), -0.4, 0.0), -0.3, 0.3)
    flow_i = jnp.clip(jax.random.uniform(key_of[2], (GRID_J, GRID_I, GRID_K, LEVELS), jnp.float32, -0.3, 0.3) * block_scale(key_of[2], (GRID_J, GRID_I, GRID_K, LEVELS), ((0, 2), (1, 4), (2, 4)), -0.4, 0.0), -0.3, 0.3)
    flow_k = jnp.clip(jax.random.uniform(key_of[3], (GRID_J, GRID_I, GRID_K, LEVELS), jnp.float32, -0.3, 0.3) * block_scale(key_of[3], (GRID_J, GRID_I, GRID_K, LEVELS), ((0, 2), (1, 4), (2, 4)), -0.4, 0.0), -0.3, 0.3)
    return {"density": density, "flow_j": flow_j, "flow_i": flow_i, "flow_k": flow_k}


def inner_cells(values, dims):
    for dim in dims:
        values = lax.slice_in_dim(values, 1, values.shape[dim] - 1, axis=dim)
    return values

def side_cells(values, dim, start, dims):
    others = [other for other in dims if other != dim]
    values = inner_cells(values, others)
    return lax.slice_in_dim(values, start, start + values.shape[dim] - 2, axis=dim)

def advance(padded, flow_j, flow_i, flow_k):
    middle = inner_cells(padded, (0, 1, 2))
    lower = [side_cells(padded, dim, 0, (0, 1, 2)) for dim in (0, 1, 2)]
    upper = [side_cells(padded, dim, 2, (0, 1, 2)) for dim in (0, 1, 2)]
    slopes = [above - below for above, below in zip(upper, lower)]
    smooth_rate = 0.05
    spread = lower[0] + upper[0] + lower[1] + upper[1] + lower[2] + upper[2] - 6.0 * middle
    return middle - flow_j * slopes[0] - flow_i * slopes[1] - flow_k * slopes[2] + smooth_rate * spread

def reference(density, flow_j, flow_i, flow_k):
    for step in range(STEPS):
        density = advance(jnp.pad(density, ((1, 1), (1, 1), (1, 1), (0, 0)), mode='constant'), flow_j, flow_i, flow_k)
    line_mean = lax.optimization_barrier(jnp.mean(density, axis=2, keepdims=True))
    centred = density - line_mean
    line_variance = lax.optimization_barrier(jnp.mean(centred * centred, axis=2, keepdims=True))
    anomaly = centred * lax.rsqrt(line_variance + 0.0001)
    return (anomaly, density)
```

```python
import functools

import jax
import jax.numpy as jnp
from jax import lax
from jax.experimental import pallas as pl
from jax.experimental.pallas import tpu as pltpu
from jax.sharding import PartitionSpec as P

STEPS = 6
CHUNK = 2
MESH = pl.DeviceIdType.MESH


def advance_kernel(
    sizes, dens, flow_j, flow_i, flow_k, out,
    st, fl, hk, sk, in_sem, fl_sem, out_sem,
    k_send, k_recv, i_send, i_recv, j_send, j_recv,
):
    n_r, n_c, n_s = sizes
    n_j, n_i, n_k, n_l = dens.shape
    chunks = n_j // CHUNK
    r, q, s = lax.axis_index("rows"), lax.axis_index("cols"), lax.axis_index("slabs")
    places = {"rows": (r, n_r), "cols": (q, n_c), "slabs": (s, n_s)}

    def sends(axis, d):
        at, count = places[axis]
        return at < count - 1 if d == 0 else at > 0

    def takes(axis, d):
        at, count = places[axis]
        return at > 0 if d == 0 else at < count - 1

    def beside(axis, d):
        at, count = places[axis]
        return {axis: jnp.minimum(at + 1, count - 1) if d == 0 else jnp.maximum(at - 1, 0)}

    def remote(src, dst, send, recv, axis, d):
        return pltpu.make_async_remote_copy(
            src_ref=src, dst_ref=dst, send_sem=send, recv_sem=recv,
            device_id=beside(axis, d), device_id_type=MESH,
        )

    def k_copy(slot, c, d):
        rows = pl.ds(c * CHUNK, CHUNK)
        return remote(
            sk.at[slot, d, rows], hk.at[slot, d, rows],
            k_send.at[slot, d, c], k_recv.at[slot, d, c], "slabs", d,
        )

    def i_copy(slot, c, d):
        rows = pl.ds(c * CHUNK + 1, CHUNK)
        src, dst = (n_i, 0) if d == 0 else (1, n_i + 1)
        return remote(
            st.at[slot, rows, src], st.at[slot, rows, dst],
            i_send.at[slot, d, c], i_recv.at[slot, d, c], "cols", d,
        )

    def j_copy(slot, d):
        src, dst = (n_j, 0) if d == 0 else (1, n_j + 1)
        cells = pl.ds(1, n_i)
        return remote(
            st.at[slot, src, cells], st.at[slot, dst, cells],
            j_send.at[slot, d], j_recv.at[slot, d], "rows", d,
        )

    def last_of(c, d):
        return c == (chunks - 1 if d == 0 else 0)

    def first_of(c, d):
        return c == (0 if d == 0 else chunks - 1)

    def start_sends(slot, c):
        for d in (0, 1):
            @pl.when(jnp.logical_and(sends("rows", d), last_of(c, d)))
            def _():
                j_copy(slot, d).start()

            @pl.when(sends("cols", d))
            def _():
                i_copy(slot, c, d).start()

            @pl.when(sends("slabs", d))
            def _():
                k_copy(slot, c, d).start()

    def wait_sends(slot, c):
        for d in (0, 1):
            @pl.when(jnp.logical_and(sends("rows", d), last_of(c, d)))
            def _():
                j_copy(slot, d).wait_send()

            @pl.when(sends("cols", d))
            def _():
                i_copy(slot, c, d).wait_send()

            @pl.when(sends("slabs", d))
            def _():
                k_copy(slot, c, d).wait_send()

    def wait_halos(slot, c):
        for d in (0, 1):
            @pl.when(jnp.logical_and(takes("rows", d), first_of(c, d)))
            def _():
                j_copy(slot, d).wait_recv()

            @pl.when(takes("cols", d))
            def _():
                i_copy(slot, c, d).wait_recv()

            @pl.when(takes("slabs", d))
            def _():
                k_copy(slot, c, d).wait_recv()

    def dens_copy(c):
        return pltpu.make_async_copy(
            dens.at[pl.ds(c * CHUNK, CHUNK)],
            st.at[0, pl.ds(c * CHUNK + 1, CHUNK), pl.ds(1, n_i)],
            in_sem.at[c],
        )

    def flow_copy(c, d):
        rows = pl.ds(c * CHUNK, CHUNK)
        return pltpu.make_async_copy(
            (flow_j, flow_i, flow_k)[d].at[rows], fl.at[d, rows], fl_sem.at[d, c]
        )

    def out_copy(c):
        return pltpu.make_async_copy(
            st.at[STEPS % 2, pl.ds(c * CHUNK + 1, CHUNK), pl.ds(1, n_i)],
            out.at[pl.ds(c * CHUNK, CHUNK)],
            out_sem.at[c],
        )

    def order(p):
        return jnp.where(lax.rem(r, 2) == 0, chunks - 1 - p, p)

    def load(p, carry):
        dens_copy(order(p)).start()
        return carry

    def load_flows(p, carry):
        for d in range(3):
            flow_copy(order(p), d).start()
        return carry

    lax.fori_loop(0, chunks, load, 0)
    lax.fori_loop(0, chunks, load_flows, 0)

    for d in (0, 1):
        @pl.when(jnp.logical_not(takes("slabs", d)))
        def _():
            def clear(j, carry):
                for slot in (0, 1):
                    hk[slot, d, j] = jnp.zeros((n_i, n_l), jnp.float32)
                return carry

            lax.fori_loop(0, n_j, clear, 0)

        @pl.when(jnp.logical_not(takes("cols", d)))
        def _():
            for slot in (0, 1):
                for j in range(n_j):
                    st[slot, j + 1, 0 if d == 0 else n_i + 1] = jnp.zeros((n_k, n_l), jnp.float32)

        @pl.when(jnp.logical_not(takes("rows", d)))
        def _():
            def clear(i, carry):
                for slot in (0, 1):
                    st[slot, 0 if d == 0 else n_j + 1, i + 1] = jnp.zeros((n_k, n_l), jnp.float32)
                return carry

            lax.fori_loop(0, n_i, clear, 0)

    barrier = pltpu.get_barrier_semaphore()
    for axis in ("rows", "cols", "slabs"):
        for d in (0, 1):
            @pl.when(sends(axis, d))
            def _():
                pl.semaphore_signal(barrier, inc=1, device_id=beside(axis, d), device_id_type=MESH)
    pl.semaphore_wait(
        barrier,
        sum(takes(axis, d).astype(jnp.int32) for axis in ("rows", "cols", "slabs") for d in (0, 1)),
    )

    group = 8 if n_i % 8 == 0 else 1

    def keep_faces(slot, j, i, value):
        sk[slot, 0, j, pl.ds(i, 1)] = value[n_k - 1:n_k]
        sk[slot, 1, j, pl.ds(i, 1)] = value[0:1]

    def first_faces(p, carry):
        c = order(p)
        dens_copy(c).wait()
        for jj in range(CHUNK):
            j = c * CHUNK + jj

            def cells(g, carry):
                i0 = pl.multiple_of(g * group, group)
                for e in range(group):
                    keep_faces(0, j, i0 + e, st[0, j + 1, i0 + e + 1])
                return carry

            lax.fori_loop(0, n_i // group, cells, 0)
        start_sends(0, c)
        return carry

    lax.fori_loop(0, chunks, first_faces, 0)

    level = lax.broadcasted_iota(jnp.int32, (n_k, n_l), 0)
    bottom, top = level == 0, level == n_k - 1

    def advance(now, later, c):
        for jj in range(CHUNK):
            j = c * CHUNK + jj

            def cells(g, carry):
                i0 = pl.multiple_of(g * group, group)
                line = [st[now, j + 1, i0 + e] for e in range(group + 2)]
                for e in range(group):
                    i = i0 + e
                    middle = line[e + 1]
                    low_i, high_i = line[e], line[e + 2]
                    low_j, high_j = st[now, j, i + 1], st[now, j + 2, i + 1]
                    low_k = jnp.where(bottom, hk[now, 0, j, pl.ds(i, 1)], pltpu.roll(middle, 1, 0))
                    high_k = jnp.where(
                        top, hk[now, 1, j, pl.ds(i, 1)], pltpu.roll(middle, n_k - 1, 0)
                    )
                    spread = low_j + high_j + low_i + high_i + low_k + high_k - 6.0 * middle
                    value = (
                        middle
                        - fl[0, j, i] * (high_j - low_j)
                        - fl[1, j, i] * (high_i - low_i)
                        - fl[2, j, i] * (high_k - low_k)
                        + 0.05 * spread
                    )
                    st[later, j + 1, i + 1] = value
                    keep_faces(later, j, i, value)
                return carry

            lax.fori_loop(0, n_i // group, cells, 0)

    def step(p, carry):
        t, c = p // chunks, order(lax.rem(p, chunks))
        now = lax.rem(t, 2)
        later = 1 - now

        @pl.when(t == 0)
        def _():
            for d in range(3):
                flow_copy(c, d).wait()

        wait_halos(now, c)

        @pl.when(t > 0)
        def _():
            wait_sends(later, c)

        advance(now, later, c)

        @pl.when(t < STEPS - 1)
        def _():
            start_sends(later, c)

        @pl.when(t == STEPS - 1)
        def _():
            out_copy(c).start()

        return carry

    lax.fori_loop(0, STEPS * chunks, step, 0)

    def finish(c, carry):
        wait_sends((STEPS - 1) % 2, c)
        out_copy(c).wait()
        return carry

    lax.fori_loop(0, chunks, finish, 0)


def body(sizes, density, flow_j, flow_i, flow_k):
    n_j, n_i, n_k, n_l = density.shape
    chunks = n_j // CHUNK
    dma = pltpu.SemaphoreType.DMA
    density = pl.pallas_call(
        functools.partial(advance_kernel, sizes),
        out_shape=jax.ShapeDtypeStruct(density.shape, density.dtype),
        in_specs=[pl.BlockSpec(memory_space=pl.ANY)] * 4,
        out_specs=pl.BlockSpec(memory_space=pl.ANY),
        scratch_shapes=[
            pltpu.VMEM((2, n_j + 2, n_i + 2, n_k, n_l), jnp.float32),
            pltpu.VMEM((3, n_j, n_i, n_k, n_l), jnp.float32),
            pltpu.VMEM((2, 2, n_j, n_i, n_l), jnp.float32),
            pltpu.VMEM((2, 2, n_j, n_i, n_l), jnp.float32),
            dma((chunks,)), dma((3, chunks)), dma((chunks,)),
            dma((2, 2, chunks)), dma((2, 2, chunks)),
            dma((2, 2, chunks)), dma((2, 2, chunks)),
            dma((2, 2)), dma((2, 2)),
        ],
        compiler_params=pltpu.CompilerParams(
            collective_id=0, has_side_effects=True, vmem_limit_bytes=60 * 1024 * 1024
        ),
    )(density, flow_j, flow_i, flow_k)
    count = density.shape[2] * lax.axis_size("slabs")
    guess = 1.0
    moved = density - guess
    totals, squares = lax.psum(
        (jnp.sum(moved, axis=2, keepdims=True), jnp.sum(moved * moved, axis=2, keepdims=True)),
        "slabs",
    )
    line_mean = guess + totals / count
    centred = density - line_mean
    line_variance = squares / count - totals / count * (totals / count)
    anomaly = centred * lax.rsqrt(line_variance + 0.0001)
    return (anomaly, density)


def solution(mesh):
    sizes = tuple(mesh.shape[axis] for axis in ("rows", "cols", "slabs"))
    spec = P("rows", "cols", "slabs", None)
    return jax.shard_map(
        functools.partial(body, sizes),
        mesh=mesh,
        in_specs=(spec,) * 4,
        out_specs=(spec,) * 2,
        check_vma=False,
    )
```

```python
import functools

import jax
import jax.numpy as jnp
from jax import lax
from jax.experimental import pallas as pl
from jax.experimental.pallas import tpu as pltpu
from jax.sharding import PartitionSpec as P

STEPS = 6
CHUNK = 2
MESH = pl.DeviceIdType.MESH


def advance_kernel(
    sizes, dens, flow_j, flow_i, flow_k, out,
    st, fl, hk, sk, in_sem, fl_sem, out_sem,
    k_send, k_recv, i_send, i_recv, j_send, j_recv,
):
    n_r, n_c, n_s = sizes
    n_j, n_i, n_k, n_l = dens.shape
    chunks = n_j // CHUNK
    r, q, s = lax.axis_index("rows"), lax.axis_index("cols"), lax.axis_index("slabs")
    places = {"rows": (r, n_r), "cols": (q, n_c), "slabs": (s, n_s)}

    def sends(axis, d):
        at, count = places[axis]
        return at < count - 1 if d == 0 else at > 0

    def takes(axis, d):
        at, count = places[axis]
        return at > 0 if d == 0 else at < count - 1

    def beside(axis, d):
        at, count = places[axis]
        return {axis: jnp.minimum(at + 1, count - 1) if d == 0 else jnp.maximum(at - 1, 0)}

    def remote(src, dst, send, recv, axis, d):
        return pltpu.make_async_remote_copy(
            src_ref=src, dst_ref=dst, send_sem=send, recv_sem=recv,
            device_id=beside(axis, d), device_id_type=MESH,
        )

    def k_copy(slot, c, d):
        rows = pl.ds(c * CHUNK, CHUNK)
        return remote(
            sk.at[slot, d, rows], hk.at[slot, d, rows],
            k_send.at[slot, d, c], k_recv.at[slot, d, c], "slabs", d,
        )

    def i_copy(slot, c, d):
        rows = pl.ds(c * CHUNK + 1, CHUNK)
        src, dst = (n_i, 0) if d == 0 else (1, n_i + 1)
        return remote(
            st.at[slot, rows, src], st.at[slot, rows, dst],
            i_send.at[slot, d, c], i_recv.at[slot, d, c], "cols", d,
        )

    def j_copy(slot, d):
        src, dst = (n_j, 0) if d == 0 else (1, n_j + 1)
        cells = pl.ds(1, n_i)
        return remote(
            st.at[slot, src, cells], st.at[slot, dst, cells],
            j_send.at[slot, d], j_recv.at[slot, d], "rows", d,
        )

    def last_of(c, d):
        return c == (chunks - 1 if d == 0 else 0)

    def first_of(c, d):
        return c == (0 if d == 0 else chunks - 1)

    def start_sends(slot, c):
        for d in (0, 1):
            @pl.when(jnp.logical_and(sends("rows", d), last_of(c, d)))
            def _():
                j_copy(slot, d).start()

            @pl.when(sends("cols", d))
            def _():
                i_copy(slot, c, d).start()

            @pl.when(sends("slabs", d))
            def _():
                k_copy(slot, c, d).start()

    def wait_sends(slot, c):
        for d in (0, 1):
            @pl.when(jnp.logical_and(sends("rows", d), last_of(c, d)))
            def _():
                j_copy(slot, d).wait_send()

            @pl.when(sends("cols", d))
            def _():
                i_copy(slot, c, d).wait_send()

            @pl.when(sends("slabs", d))
            def _():
                k_copy(slot, c, d).wait_send()

    def wait_halos(slot, c):
        for d in (0, 1):
            @pl.when(jnp.logical_and(takes("rows", d), first_of(c, d)))
            def _():
                j_copy(slot, d).wait_recv()

            @pl.when(takes("cols", d))
            def _():
                i_copy(slot, c, d).wait_recv()

            @pl.when(takes("slabs", d))
            def _():
                k_copy(slot, c, d).wait_recv()

    def dens_copy(c):
        return pltpu.make_async_copy(
            dens.at[pl.ds(c * CHUNK, CHUNK)],
            st.at[0, pl.ds(c * CHUNK + 1, CHUNK), pl.ds(1, n_i)],
            in_sem.at[c],
        )

    def flow_copy(c, d):
        rows = pl.ds(c * CHUNK, CHUNK)
        return pltpu.make_async_copy(
            (flow_j, flow_i, flow_k)[d].at[rows], fl.at[d, rows], fl_sem.at[d, c]
        )

    def out_copy(c):
        return pltpu.make_async_copy(
            st.at[STEPS % 2, pl.ds(c * CHUNK + 1, CHUNK), pl.ds(1, n_i)],
            out.at[pl.ds(c * CHUNK, CHUNK)],
            out_sem.at[c],
        )

    def order(p):
        return jnp.where(lax.rem(r, 2) == 0, chunks - 1 - p, p)

    def load(p, carry):
        dens_copy(order(p)).start()
        return carry

    def load_flows(p, carry):
        for d in range(3):
            flow_copy(order(p), d).start()
        return carry

    lax.fori_loop(0, chunks, load, 0)
    lax.fori_loop(0, chunks, load_flows, 0)

    for d in (0, 1):
        @pl.when(jnp.logical_not(takes("slabs", d)))
        def _():
            def clear(j, carry):
                for slot in (0, 1):
                    hk[slot, d, j] = jnp.zeros((n_i, n_l), jnp.float32)
                return carry

            lax.fori_loop(0, n_j, clear, 0)

        @pl.when(jnp.logical_not(takes("cols", d)))
        def _():
            for slot in (0, 1):
                for j in range(n_j):
                    st[slot, j + 1, 0 if d == 0 else n_i + 1] = jnp.zeros((n_k, n_l), jnp.float32)

        @pl.when(jnp.logical_not(takes("rows", d)))
        def _():
            def clear(i, carry):
                for slot in (0, 1):
                    st[slot, 0 if d == 0 else n_j + 1, i + 1] = jnp.zeros((n_k, n_l), jnp.float32)
                return carry

            lax.fori_loop(0, n_i, clear, 0)

    barrier = pltpu.get_barrier_semaphore()
    for axis in ("rows", "cols", "slabs"):
        for d in (0, 1):
            @pl.when(sends(axis, d))
            def _():
                pl.semaphore_signal(barrier, inc=1, device_id=beside(axis, d), device_id_type=MESH)
    pl.semaphore_wait(
        barrier,
        sum(takes(axis, d).astype(jnp.int32) for axis in ("rows", "cols", "slabs") for d in (0, 1)),
    )

    group = 8 if n_i % 8 == 0 else 1

    def keep_faces(slot, j, i, value):
        sk[slot, 0, j, pl.ds(i, 1)] = value[n_k - 1:n_k]
        sk[slot, 1, j, pl.ds(i, 1)] = value[0:1]

    def first_faces(p, carry):
        c = order(p)
        dens_copy(c).wait()
        for jj in range(CHUNK):
            j = c * CHUNK + jj

            def cells(g, carry):
                i0 = pl.multiple_of(g * group, group)
                for e in range(group):
                    keep_faces(0, j, i0 + e, st[0, j + 1, i0 + e + 1])
                return carry

            lax.fori_loop(0, n_i // group, cells, 0)
        start_sends(0, c)
        return carry

    lax.fori_loop(0, chunks, first_faces, 0)

    level = lax.broadcasted_iota(jnp.int32, (n_k, n_l), 0)
    bottom, top = level == 0, level == n_k - 1

    def advance(now, later, c):
        for jj in range(CHUNK):
            j = c * CHUNK + jj

            def cells(g, carry):
                i0 = pl.multiple_of(g * group, group)
                line = [st[now, j + 1, i0 + e] for e in range(group + 2)]
                for e in range(group):
                    i = i0 + e
                    middle = line[e + 1]
                    low_i, high_i = line[e], line[e + 2]
                    low_j, high_j = st[now, j, i + 1], st[now, j + 2, i + 1]
                    low_k = jnp.where(bottom, hk[now, 0, j, pl.ds(i, 1)], pltpu.roll(middle, 1, 0))
                    high_k = jnp.where(
                        top, hk[now, 1, j, pl.ds(i, 1)], pltpu.roll(middle, n_k - 1, 0)
                    )
                    spread = low_j + high_j + low_i + high_i + low_k + high_k - 6.0 * middle
                    value = (
                        middle
                        - fl[0, j, i] * (high_j - low_j)
                        - fl[1, j, i] * (high_i - low_i)
                        - fl[2, j, i] * (high_k - low_k)
                        + 0.05 * spread
                    )
                    st[later, j + 1, i + 1] = value
                    keep_faces(later, j, i, value)
                return carry

            lax.fori_loop(0, n_i // group, cells, 0)

    def step(p, carry):
        t, c = p // chunks, order(lax.rem(p, chunks))
        now = lax.rem(t, 2)
        later = 1 - now

        @pl.when(t == 0)
        def _():
            for d in range(3):
                flow_copy(c, d).wait()

        wait_halos(now, c)

        @pl.when(t > 0)
        def _():
            wait_sends(later, c)

        advance(now, later, c)

        @pl.when(t < STEPS - 1)
        def _():
            start_sends(later, c)

        @pl.when(t == STEPS - 1)
        def _():
            out_copy(c).start()

        return carry

    lax.fori_loop(0, STEPS * chunks, step, 0)

    def finish(c, carry):
        wait_sends((STEPS - 1) % 2, c)
        out_copy(c).wait()
        return carry

    lax.fori_loop(0, chunks, finish, 0)


def line_sums(totals, squares):
    if lax.axis_size("slabs") != 4 or totals.shape[1] % 2:
        return lax.psum((totals, squares), "slabs")
    s = lax.axis_index("slabs")

    def swap(values, bit):
        return lax.ppermute(values, "slabs", [(i, i ^ bit) for i in range(4)])

    half = totals.shape[1] // 2
    found = []
    for start, first, second in ((0, 1, 2), (half, 2, 1)):
        total, square = (
            lax.slice_in_dim(values, start, start + half, axis=1) for values in (totals, squares)
        )
        low = (s // first) % 2 == 0
        part = jnp.where(low, total, square) + swap(jnp.where(low, square, total), first)
        part = part + swap(part, second)
        other = swap(part, first)
        found.append((jnp.where(low, part, other), jnp.where(low, other, part)))
    return [jnp.concatenate(pair, axis=1) for pair in zip(*found)]


def body(sizes, density, flow_j, flow_i, flow_k):
    n_j, n_i, n_k, n_l = density.shape
    chunks = n_j // CHUNK
    dma = pltpu.SemaphoreType.DMA
    density = pl.pallas_call(
        functools.partial(advance_kernel, sizes),
        out_shape=jax.ShapeDtypeStruct(density.shape, density.dtype),
        in_specs=[pl.BlockSpec(memory_space=pl.ANY)] * 4,
        out_specs=pl.BlockSpec(memory_space=pl.ANY),
        scratch_shapes=[
            pltpu.VMEM((2, n_j + 2, n_i + 2, n_k, n_l), jnp.float32),
            pltpu.VMEM((3, n_j, n_i, n_k, n_l), jnp.float32),
            pltpu.VMEM((2, 2, n_j, n_i, n_l), jnp.float32),
            pltpu.VMEM((2, 2, n_j, n_i, n_l), jnp.float32),
            dma((chunks,)), dma((3, chunks)), dma((chunks,)),
            dma((2, 2, chunks)), dma((2, 2, chunks)),
            dma((2, 2, chunks)), dma((2, 2, chunks)),
            dma((2, 2)), dma((2, 2)),
        ],
        compiler_params=pltpu.CompilerParams(
            collective_id=0, has_side_effects=True, vmem_limit_bytes=60 * 1024 * 1024
        ),
    )(density, flow_j, flow_i, flow_k)
    count = density.shape[2] * lax.axis_size("slabs")
    guess = 1.0
    moved = density - guess
    totals, squares = line_sums(
        jnp.sum(moved, axis=2, keepdims=True), jnp.sum(moved * moved, axis=2, keepdims=True)
    )
    line_mean = guess + totals / count
    centred = density - line_mean
    line_variance = squares / count - totals / count * (totals / count)
    anomaly = centred * lax.rsqrt(line_variance + 0.0001)
    return (anomaly, density)


def solution(mesh):
    sizes = tuple(mesh.shape[axis] for axis in ("rows", "cols", "slabs"))
    spec = P("rows", "cols", "slabs", None)
    return jax.shard_map(
        functools.partial(body, sizes),
        mesh=mesh,
        in_specs=(spec,) * 4,
        out_specs=(spec,) * 2,
        check_vma=False,
    )
```
